32 devices in a mesh: mat: 4 (over z), tile: 8 (over y, x, core).
Axes of the slice: x: 2, y: 2, z: 4, core: 2. Of those that a mesh axis runs over, the one named last changes fastest.
Arguments:
- volume: bfloat16 [4, 64, 8, 1024], P('mat', None, 'tile'), may hold values from -4 to 4
- system: bfloat16 [8, 1024, 32, 128], P('tile'), may hold values from 0 to 0.026977539
- geometry: int32 [8, 16], replicated, may hold values from 0 to 2
- attenuation: float32 [4, 64], replicated, may hold values from 0.05 to 0.5
- response: float32 [8, 64], replicated, may hold values from 0.002 to 0.06
- crosstalk: float32 [8], replicated, may hold values from 0.04 to 0.24
Outputs:
- counts: float32 [8, 64, 16, 512], P(None, ('mat', 'tile'))
The draws below stay inside these ranges and needn't reach their ends.
Inputs may be any that keep to these rules, and one draw needn't show every extreme that they name: A tile touches, in view v, exactly the 2 detector blocks geometry[t, v] to geometry[t, v] + 1.
All inputs are finite; a program needn't handle non-finite values.
Results may differ from the reference program's by a relative error of at most 0.0003.
Values may be sent and summed in bfloat16 or wider, within the bound.
A program may use at most 128 MiB of HBM per device.

```python
import math
import jax
import jax.numpy as jnp
from jax import lax

MATS = 4
TILE_VOX = 1024
VIEWS = 16
PIXELS = 512
PB = 128
TOUCH = 2
EBINS = 64
CBINS = 8
TILES = 8
SLICES = 64
PBLK = 4
KT = 32
RAYS = 8192


def place_ends(entries, rng, least, largest):
    shape = entries.shape
    place = [jax.random.randint(jax.random.fold_in(rng, axis), (), 0, shape[axis]) for axis in range(len(shape))]
    entries = entries.at[tuple(place)].set(least)
    longest = shape.index(max(shape))
    place[longest] = (place[longest] + 1) % shape[longest]
    return entries.at[tuple(place)].set(largest)


def level_of(stream_key, shape, cuts, low, high):
    level = 1.0
    for dim, shards_of in cuts:
        steps = jax.random.uniform(jax.random.fold_in(jax.random.fold_in(stream_key, 6), dim), (shards_of,), jnp.float32, low / len(cuts), high / len(cuts))
        level = level * jnp.repeat(jnp.exp(steps), shape[dim] // shards_of).reshape((-1,) + (1,) * (len(shape) - 1 - dim))
    return level


def noise(own_key, extent, width, bound, split=(), kind=jnp.bfloat16):
    values = jax.random.normal(own_key, extent, jnp.float32) * width
    if len(split) > 0:
        values = level_of(own_key, extent, split, -0.22, 0.18) * values
    return jnp.clip(values, min=-bound, max=bound).astype(kind)


def setup_inputs(seed: int = 0) -> dict:
    arg_keys = jax.random.split(jax.random.key(seed), 7)
    volume = noise(arg_keys[0], (MATS, SLICES, TILES, TILE_VOX), 1.0, 4.0, ((0, 4), (2, 8)))
    system = jnp.clip(0.026977539 * jax.random.uniform(arg_keys[1], (TILES, TILE_VOX, KT, PB), jnp.float32) ** level_of(arg_keys[1], (TILES, TILE_VOX, KT, PB), ((0, 8),), -0.2, 0.2), 0.0, 0.026977539).astype(jnp.bfloat16)
    geometry = place_ends(jax.random.randint(arg_keys[2], (TILES, VIEWS), 0, PBLK - TOUCH + 1), jax.random.fold_in(arg_keys[2], 1), 0, PBLK - TOUCH).astype(jnp.int32)
    attenuation = jnp.clip(jnp.exp(jax.random.uniform(arg_keys[3], (MATS, EBINS), jnp.float32, math.log(0.05), math.log(0.5))), 0.05, 0.5)
    response = jnp.clip(jnp.exp(jax.random.uniform(arg_keys[4], (CBINS, EBINS), jnp.float32, math.log(0.002), math.log(0.06))), 0.002, 0.06)
    crosstalk = jnp.clip(jax.random.uniform(arg_keys[5], (CBINS,), jnp.float32, 0.04, 0.24), 0.04, 0.24)
    return {"volume": volume, "system": system, "geometry": geometry, "attenuation": attenuation, "response": response, "crosstalk": crosstalk}


def reference(volume, system, geometry, attenuation, response, crosstalk):
    row_total = MATS * SLICES
    block_ids = jnp.arange(PBLK, dtype=jnp.int32)
    touch_ids = jnp.arange(TOUCH, dtype=jnp.int32)

    def one_tile(running, tile_index):
        columns = lax.dynamic_index_in_dim(volume, tile_index, 2, keepdims=False)
        columns = columns.reshape(row_total, TILE_VOX).astype(jnp.float32)
        matrix = lax.dynamic_index_in_dim(system, tile_index, 0, keepdims=False)
        matrix = matrix.reshape(TILE_VOX, KT * PB).astype(jnp.float32)
        partial_value = jnp.dot(columns, matrix, preferred_element_type=jnp.float32, precision=lax.Precision.HIGHEST)
        partial_value = partial_value.reshape(row_total, VIEWS, TOUCH, PB)
        first_block = lax.dynamic_index_in_dim(geometry, tile_index, 0, keepdims=False)
        placed = (first_block[:, None, None] + touch_ids[None, :, None] == block_ids[None, None, :]).astype(jnp.float32)
        expanded = jnp.einsum('rvjp,vjb->rvbp', partial_value, placed, precision=lax.Precision.HIGHEST)
        return (running + expanded, None)
    start_sums = jnp.zeros((row_total, VIEWS, PBLK, PB), jnp.float32)
    summed = lax.scan(one_tile, start_sums, jnp.arange(TILES, dtype=jnp.int32))[0]
    proj = summed.reshape(MATS, SLICES, RAYS).transpose(1, 0, 2)

    def one_row(integrals):
        exponent = jnp.dot(attenuation.T, integrals, preferred_element_type=jnp.float32, precision=lax.Precision.HIGHEST)
        return jnp.dot(response, jnp.exp(-exponent), preferred_element_type=jnp.float32, precision=lax.Precision.HIGHEST)
    detected = lax.map(one_row, proj).transpose(1, 0, 2)
    padded = jnp.pad(detected, ((0, 0), (1, 1), (0, 0)))
    leakage = crosstalk[:, None, None]
    counts = (1.0 - 2.0 * leakage) * detected + leakage * (padded[:, :-2] + padded[:, 2:])
    return counts.reshape(CBINS, SLICES, VIEWS, PIXELS)
```

```python
import functools

import jax
import jax.numpy as jnp
import numpy as np
from jax import lax
from jax.experimental import pallas as pl
from jax.experimental.pallas import tpu as pltpu
from jax.sharding import PartitionSpec as P

PIXELS = 512
GROUPS = 4
LOG2E = 1.4426950408889634
MESH = pl.DeviceIdType.MESH
LINK = jnp.float32


def loop(low, high, body):
    if high - low <= 8:
        for index in range(low, high):
            body(index)
    else:
        lax.fori_loop(low, high, lambda index, _: (body(index), 0)[1], 0)


def kernel(mats, tiles, slices, voxels, views, touch, pb, pblk, ebins, cbins,
           order_ref, volume_ref, system_ref, geometry_ref, attenuation_ref, response_ref, crosstalk_ref,
           counts_ref,
           matrix, permuted, partial_out, partial_in, summed_out, summed_in, detected, before, after,
           matrix_sem, send1, recv1, send2, recv2, send3, recv3):
    me_mat, me_tile = lax.axis_index("mat"), lax.axis_index("tile")
    devices = mats * tiles
    me = me_mat * tiles + me_tile
    rows = slices // devices
    share = mats * rows
    group_views = views // GROUPS
    group_cols = group_views * touch
    rays = group_views * pblk
    has_prev, has_next = me > 0, me < devices - 1
    up, down = me + 1, me - 1

    loads = [
        pltpu.make_async_copy(system_ref.at[:, pl.ds(g * group_cols, group_cols)], matrix.at[g], matrix_sem.at[g])
        for g in range(GROUPS)
    ]
    for load in loads:
        load.start()

    barrier = pltpu.get_barrier_semaphore()

    def greet_tile(off):
        pl.semaphore_signal(barrier, inc=1, device_id={"tile": lax.rem(me_tile + off, tiles)}, device_id_type=MESH)

    def greet_mat(off):
        pl.semaphore_signal(barrier, inc=1, device_id={"mat": lax.rem(me_mat + off, mats)}, device_id_type=MESH)

    def place(device):
        return {"mat": device // tiles, "tile": lax.rem(device, tiles)}

    loop(1, tiles, greet_tile)
    loop(1, mats, greet_mat)

    @pl.when(has_prev)
    def _():
        pl.semaphore_signal(barrier, inc=1, device_id=place(down), device_id_type=MESH)

    @pl.when(has_next)
    def _():
        pl.semaphore_signal(barrier, inc=1, device_id=place(up), device_id_type=MESH)

    permuted[...] = jnp.dot(order_ref[...], volume_ref[...], preferred_element_type=jnp.float32).astype(jnp.bfloat16)

    def copy1(g, off):
        peer = lax.rem(me_tile + off, tiles)
        return pltpu.make_async_remote_copy(
            src_ref=partial_out.at[g, peer], dst_ref=partial_in.at[g, me_tile],
            send_sem=send1.at[g, peer], recv_sem=recv1.at[g, me_tile],
            device_id={"tile": peer}, device_id_type=MESH)

    def arrival1(g, off):
        peer = lax.rem(me_tile + off, tiles)
        return pltpu.make_async_remote_copy(
            src_ref=partial_out.at[g, peer], dst_ref=partial_in.at[g, peer],
            send_sem=send1.at[g, peer], recv_sem=recv1.at[g, peer],
            device_id={"tile": peer}, device_id_type=MESH)

    def copy2(g, off):
        peer = lax.rem(me_mat + off, mats)
        return pltpu.make_async_remote_copy(
            src_ref=summed_out.at[g, peer], dst_ref=summed_in.at[g, me_mat],
            send_sem=send2.at[g, peer], recv_sem=recv2.at[g, me_mat],
            device_id={"mat": peer}, device_id_type=MESH)

    def arrival2(g, off):
        peer = lax.rem(me_mat + off, mats)
        return pltpu.make_async_remote_copy(
            src_ref=summed_out.at[g, peer], dst_ref=summed_in.at[g, peer],
            send_sem=send2.at[g, peer], recv_sem=recv2.at[g, peer],
            device_id={"mat": peer}, device_id_type=MESH)

    def copy_down(g):
        return pltpu.make_async_remote_copy(
            src_ref=detected.at[g, 0], dst_ref=after.at[g],
            send_sem=send3.at[g, 0], recv_sem=recv3.at[g, 0],
            device_id=place(down), device_id_type=MESH)

    def copy_up(g):
        return pltpu.make_async_remote_copy(
            src_ref=detected.at[g, rows - 1], dst_ref=before.at[g],
            send_sem=send3.at[g, 1], recv_sem=recv3.at[g, 1],
            device_id=place(up), device_id_type=MESH)

    def multiply(g):
        loads[g].wait()
        columns = jnp.swapaxes(matrix[g], 0, 1)
        for k in range(0, group_cols, 2):
            pair = jnp.concatenate([columns[k], columns[k + 1]], axis=-1)
            product = jnp.dot(permuted[...], pair, preferred_element_type=jnp.float32)
            product = product.reshape(tiles, share, 2 * pb)
            partial_out[g, :, k] = product[:, :, :pb].astype(LINK)
            partial_out[g, :, k + 1] = product[:, :, pb:].astype(LINK)
        if g == 0:
            pl.semaphore_wait(
                barrier, tiles - 1 + mats - 1 + has_prev.astype(jnp.int32) + has_next.astype(jnp.int32))
        loop(1, tiles, lambda off: copy1(g, off).start())
        partial_in[g, me_tile] = partial_out[g, me_tile]

    def add_tiles(g):
        loop(1, tiles, lambda off: arrival1(g, off).wait_recv())

        def add(tile, sums):
            sums = list(sums)
            for v in range(group_views):
                first = geometry_ref[tile, g * group_views + v]
                for j in range(touch):
                    value = partial_in[g, tile, v * touch + j].astype(jnp.float32)
                    for b in range(j, pblk - touch + 1 + j):
                        weight = (first + j == b).astype(jnp.float32)
                        sums[b * group_views + v] += weight * value
            return tuple(sums)

        sums = tuple(jnp.zeros((share, pb), jnp.float32) for _ in range(rays))
        if tiles <= 8:
            for tile in range(tiles):
                sums = add(tile, sums)
        else:
            sums = lax.fori_loop(0, tiles, add, sums)
        by_row = jnp.swapaxes(jnp.stack(sums, axis=0), 0, 1)
        summed_out[g] = by_row.reshape(mats, rows, rays, pb).astype(LINK)
        loop(1, mats, lambda off: copy2(g, off).start())
        summed_in[g, me_mat] = summed_out[g, me_mat]

    def detect(g):
        loop(1, mats, lambda off: arrival2(g, off).wait_recv())
        scaled = [summed_in[g, m].astype(jnp.float32).reshape(rows * rays, pb) * (-LOG2E) for m in range(mats)]
        unroll = 8

        def energies(block, totals):
            totals = list(totals)
            for inner in range(unroll):
                e = block * unroll + inner
                power = attenuation_ref[0, e] * scaled[0]
                for m in range(1, mats):
                    power += attenuation_ref[m, e] * scaled[m]
                passed = jnp.exp2(power)
                for b in range(cbins):
                    totals[b] += response_ref[b, e] * passed
            return tuple(totals)

        totals = tuple(jnp.zeros((rows * rays, pb), jnp.float32) for _ in range(cbins))
        totals = lax.fori_loop(0, ebins // unroll, energies, totals)
        for b in range(cbins):
            for r in range(rows):
                detected[g, r, b] = totals[b][r * rays:(r + 1) * rays]

        @pl.when(has_prev)
        def _():
            copy_down(g).start()

        @pl.when(has_next)
        def _():
            copy_up(g).start()

    def count(g):
        @pl.when(has_prev)
        def _():
            copy_up(g).wait_recv()

        @pl.when(has_next)
        def _():
            copy_down(g).wait_recv()

        for b in range(cbins):
            leak = crosstalk_ref[b]
            keep = 1.0 - 2.0 * leak
            for r in range(rows):
                lower = detected[g, r - 1, b] if r > 0 else before[g, b]
                upper = detected[g, r + 1, b] if r < rows - 1 else after[g, b]
                value = keep * detected[g, r, b] + leak * (lower + upper)
                for k in range(pblk):
                    counts_ref[b, r, g * group_views:(g + 1) * group_views, k * pb:(k + 1) * pb] = (
                        value[k * group_views:(k + 1) * group_views])

    @pl.when(jnp.logical_not(has_prev))
    def _():
        before[...] = jnp.zeros_like(before)

    @pl.when(jnp.logical_not(has_next))
    def _():
        after[...] = jnp.zeros_like(after)

    multiply(0)
    multiply(1)
    multiply(2)
    add_tiles(0)
    multiply(3)
    add_tiles(1)
    detect(0)
    add_tiles(2)
    detect(1)
    add_tiles(3)
    detect(2)
    detect(3)
    for g in range(GROUPS):
        count(g)
    for g in range(GROUPS):
        loop(1, tiles, lambda off: copy1(g, off).wait_send())
        loop(1, mats, lambda off: copy2(g, off).wait_send())

        @pl.when(has_prev)
        def _():
            copy_down(g).wait_send()

        @pl.when(has_next)
        def _():
            copy_up(g).wait_send()


def per_device(mats, tiles, volume, system, geometry, attenuation, response, crosstalk):
    slices, voxels = volume.shape[1], volume.shape[3]
    views = geometry.shape[1]
    columns, pb = system.shape[2], system.shape[3]
    touch = columns // views
    pblk = PIXELS // pb
    ebins, cbins = attenuation.shape[1], response.shape[0]
    rows = slices // (mats * tiles)
    share = mats * rows
    group_views = views // GROUPS
    rays = group_views * pblk
    source = np.arange(slices).reshape(mats, tiles, rows).transpose(1, 0, 2).reshape(-1)
    order = jnp.asarray(np.eye(slices, dtype=np.float32)[source], jnp.bfloat16)
    vmem = pl.BlockSpec(memory_space=pltpu.VMEM)
    smem = pl.BlockSpec(memory_space=pltpu.SMEM)
    dma = pltpu.SemaphoreType.DMA
    return pl.pallas_call(
        functools.partial(kernel, mats, tiles, slices, voxels, views, touch, pb, pblk, ebins, cbins),
        out_shape=jax.ShapeDtypeStruct((cbins, rows, views, PIXELS), jnp.float32),
        in_specs=[vmem, vmem, pl.BlockSpec(memory_space=pl.ANY), smem, smem, smem, smem],
        out_specs=vmem,
        scratch_shapes=[
            pltpu.VMEM((GROUPS, voxels, columns // GROUPS, pb), jnp.bfloat16),
            pltpu.VMEM((slices, voxels), jnp.bfloat16),
            pltpu.VMEM((GROUPS, tiles, columns // GROUPS, share, pb), LINK),
            pltpu.VMEM((GROUPS, tiles, columns // GROUPS, share, pb), LINK),
            pltpu.VMEM((GROUPS, mats, rows, rays, pb), LINK),
            pltpu.VMEM((GROUPS, mats, rows, rays, pb), LINK),
            pltpu.VMEM((GROUPS, rows, cbins, rays, pb), jnp.float32),
            pltpu.VMEM((GROUPS, cbins, rays, pb), jnp.float32),
            pltpu.VMEM((GROUPS, cbins, rays, pb), jnp.float32),
            dma((GROUPS,)),
            dma((GROUPS, tiles)),
            dma((GROUPS, tiles)),
            dma((GROUPS, mats)),
            dma((GROUPS, mats)),
            dma((GROUPS, 2)),
            dma((GROUPS, 2)),
        ],
        compiler_params=pltpu.CompilerParams(
            collective_id=0, has_side_effects=True, vmem_limit_bytes=60 * 2**20
        ),
        name="project",
    )(order, volume.reshape(slices, voxels), system.reshape(voxels, columns, pb), geometry, attenuation,
      response, crosstalk)


def solution(mesh):
    in_specs = (P("mat", None, "tile", None), P("tile", None, None, None), P(), P(), P(), P())
    out_specs = P(None, ("mat", "tile"), None, None)
    body = functools.partial(per_device, mesh.shape["mat"], mesh.shape["tile"])
    return jax.shard_map(body, mesh=mesh, in_specs=in_specs, out_specs=out_specs, check_vma=False)
```

```python
import functools

import jax
import jax.numpy as jnp
from jax import lax
from jax.experimental import pallas as pl
from jax.experimental.pallas import tpu as pltpu
from jax.sharding import PartitionSpec as P

PIXELS = 512
GROUPS = 4
EARLY = 2
LOG2E = 1.4426950408889634
MESH = pl.DeviceIdType.MESH


def loop(low, high, body):
    if high - low <= 8:
        for index in range(low, high):
            body(index)
    else:
        lax.fori_loop(low, high, lambda index, _: (body(index), 0)[1], 0)


def kernel(mats, tiles, slices, voxels, views, touch, pb, pblk, ebins, cbins,
           volume_ref, system_ref, geometry_ref, attenuation_ref, response_ref, crosstalk_ref,
           counts_ref,
           matrix, gathered, partial_out, partial_in, summed_out, summed_in, detected, before, after,
           matrix_sem, send0, recv0, send1, recv1, send2, recv2, send3, recv3):
    me_mat, me_tile = lax.axis_index("mat"), lax.axis_index("tile")
    devices = mats * tiles
    me = me_mat * tiles + me_tile
    rows = slices // devices
    group_views = views // GROUPS
    group_cols = group_views * touch
    rays = group_views * pblk
    has_prev, has_next = me > 0, me < devices - 1
    up, down = me + 1, me - 1

    loads = [
        pltpu.make_async_copy(system_ref.at[:, pl.ds(g * group_cols, group_cols)], matrix.at[g], matrix_sem.at[g])
        for g in range(GROUPS)
    ]
    for load in loads:
        load.start()

    barrier = pltpu.get_barrier_semaphore()

    def greet_tile(off):
        pl.semaphore_signal(barrier, inc=1, device_id={"tile": lax.rem(me_tile + off, tiles)}, device_id_type=MESH)

    def greet_mat(off):
        pl.semaphore_signal(barrier, inc=1, device_id={"mat": lax.rem(me_mat + off, mats)}, device_id_type=MESH)

    def place(device):
        return {"mat": device // tiles, "tile": lax.rem(device, tiles)}

    loop(1, tiles, greet_tile)
    loop(1, mats, greet_mat)

    @pl.when(has_prev)
    def _():
        pl.semaphore_signal(barrier, inc=1, device_id=place(down), device_id_type=MESH)

    @pl.when(has_next)
    def _():
        pl.semaphore_signal(barrier, inc=1, device_id=place(up), device_id_type=MESH)

    gathered[me_mat] = volume_ref[me_mat]

    def copy0(off):
        peer = lax.rem(me_mat + off, mats)
        return pltpu.make_async_remote_copy(
            src_ref=volume_ref.at[peer], dst_ref=gathered.at[me_mat],
            send_sem=send0.at[peer], recv_sem=recv0.at[me_mat],
            device_id={"mat": peer}, device_id_type=MESH)

    def arrival0(off):
        peer = lax.rem(me_mat + off, mats)
        return pltpu.make_async_remote_copy(
            src_ref=volume_ref.at[peer], dst_ref=gathered.at[peer],
            send_sem=send0.at[peer], recv_sem=recv0.at[peer],
            device_id={"mat": peer}, device_id_type=MESH)

    def copy1(g, off):
        peer = lax.rem(me_tile + off, tiles)
        return pltpu.make_async_remote_copy(
            src_ref=partial_out.at[g, peer], dst_ref=partial_in.at[g, me_tile],
            send_sem=send1.at[g, peer], recv_sem=recv1.at[g, me_tile],
            device_id={"tile": peer}, device_id_type=MESH)

    def arrival1(g, off):
        peer = lax.rem(me_tile + off, tiles)
        return pltpu.make_async_remote_copy(
            src_ref=partial_out.at[g, peer], dst_ref=partial_in.at[g, peer],
            send_sem=send1.at[g, peer], recv_sem=recv1.at[g, peer],
            device_id={"tile": peer}, device_id_type=MESH)

    def copy2(g, off):
        peer = lax.rem(me_mat + off, mats)
        return pltpu.make_async_remote_copy(
            src_ref=summed_out.at[g, peer], dst_ref=summed_in.at[g, me_mat],
            send_sem=send2.at[g, peer], recv_sem=recv2.at[g, me_mat],
            device_id={"mat": peer}, device_id_type=MESH)

    def arrival2(g, off):
        peer = lax.rem(me_mat + off, mats)
        return pltpu.make_async_remote_copy(
            src_ref=summed_out.at[g, peer], dst_ref=summed_in.at[g, peer],
            send_sem=send2.at[g, peer], recv_sem=recv2.at[g, peer],
            device_id={"mat": peer}, device_id_type=MESH)

    def copy_down(g):
        return pltpu.make_async_remote_copy(
            src_ref=detected.at[g, 0], dst_ref=after.at[g],
            send_sem=send3.at[g, 0], recv_sem=recv3.at[g, 0],
            device_id=place(down), device_id_type=MESH)

    def copy_up(g):
        return pltpu.make_async_remote_copy(
            src_ref=detected.at[g, rows - 1], dst_ref=before.at[g],
            send_sem=send3.at[g, 1], recv_sem=recv3.at[g, 1],
            device_id=place(up), device_id_type=MESH)

    def multiply(g):
        loads[g].wait()
        columns = jnp.swapaxes(matrix[g], 0, 1)
        if g == 0:
            pl.semaphore_wait(
                barrier, tiles - 1 + mats - 1 + has_prev.astype(jnp.int32) + has_next.astype(jnp.int32))
            loop(1, mats, lambda off: copy0(off).start())
        if g == EARLY:
            loop(1, mats, lambda off: arrival0(off).wait_recv())
        source = volume_ref if g < EARLY else gathered
        rows_in = source[...].reshape(slices, voxels)
        products = [None] * group_cols
        for k in range(0, group_cols, 2):
            pair = jnp.concatenate([columns[k], columns[k + 1]], axis=-1)
            product = jnp.dot(rows_in, pair, preferred_element_type=jnp.float32)
            for i in range(2):
                v, j = divmod(k + i, touch)
                products[j * group_views + v] = product[:, i * pb:(i + 1) * pb]
        by_row = jnp.swapaxes(jnp.stack(products, axis=0), 0, 1)
        by_row = by_row.reshape(mats, tiles, rows, group_cols, pb)
        for m in range(mats):
            partial_out[g, :, m] = by_row[m]
        loop(1, tiles, lambda off: copy1(g, off).start())
        partial_in[g, me_tile] = partial_out[g, me_tile]

    def add_tiles(g):
        loop(1, tiles, lambda off: arrival1(g, off).wait_recv())

        sublane = lax.broadcasted_iota(jnp.int32, (group_cols, pb), 0)
        view = lax.rem(sublane, group_views)
        half = sublane < group_views

        def add(tile, sums):
            sums = list(sums)
            first = jnp.full((group_cols, pb), geometry_ref[tile, g * group_views], jnp.int32)
            for v in range(1, group_views):
                first = jnp.where(view == v, geometry_ref[tile, g * group_views + v], first)
            low, middle, high = first == 0, first == 1, first == 2
            low_turned = jnp.logical_and(middle, jnp.logical_not(half))
            high_turned = jnp.logical_and(middle, half)
            for m in range(mats):
                for r in range(rows):
                    value = partial_in[g, tile, m, r]
                    turned = jnp.concatenate([value[group_views:], value[:group_views]], axis=0)
                    at = 2 * (m * rows + r)
                    sums[at] += jnp.where(low, value, jnp.where(low_turned, turned, 0.0))
                    sums[at + 1] += jnp.where(high, value, jnp.where(high_turned, turned, 0.0))
            return tuple(sums)

        sums = tuple(jnp.zeros((group_cols, pb), jnp.float32) for _ in range(2 * mats * rows))
        if tiles <= 8:
            for tile in range(tiles):
                sums = add(tile, sums)
        else:
            sums = lax.fori_loop(0, tiles, add, sums)
        target = summed_out if g < EARLY else summed_in
        for m in range(mats):
            for r in range(rows):
                at = 2 * (m * rows + r)
                target[g, m, r, :group_cols] = sums[at]
                target[g, m, r, group_cols:] = sums[at + 1]
        if g < EARLY:
            loop(1, mats, lambda off: copy2(g, off).start())
            summed_in[g, me_mat] = summed_out[g, me_mat]

    def detect(g):
        if g < EARLY:
            loop(1, mats, lambda off: arrival2(g, off).wait_recv())
        scaled = [summed_in[g, m].reshape(rows * rays, pb) * (-LOG2E) for m in range(mats)]
        unroll = 8

        def energies(block, totals):
            totals = list(totals)
            for inner in range(unroll):
                e = block * unroll + inner
                power = attenuation_ref[0, e] * scaled[0]
                for m in range(1, mats):
                    power += attenuation_ref[m, e] * scaled[m]
                passed = jnp.exp2(power)
                for b in range(cbins):
                    totals[b] += response_ref[b, e] * passed
            return tuple(totals)

        totals = tuple(jnp.zeros((rows * rays, pb), jnp.float32) for _ in range(cbins))
        totals = lax.fori_loop(0, ebins // unroll, energies, totals)
        for b in range(cbins):
            for r in range(rows):
                detected[g, r, b] = totals[b][r * rays:(r + 1) * rays]

        @pl.when(has_prev)
        def _():
            copy_down(g).start()

        @pl.when(has_next)
        def _():
            copy_up(g).start()

    def count(g):
        @pl.when(has_prev)
        def _():
            copy_up(g).wait_recv()

        @pl.when(has_next)
        def _():
            copy_down(g).wait_recv()

        for b in range(cbins):
            leak = crosstalk_ref[b]
            keep = 1.0 - 2.0 * leak
            for r in range(rows):
                lower = detected[g, r - 1, b] if r > 0 else before[g, b]
                upper = detected[g, r + 1, b] if r < rows - 1 else after[g, b]
                value = keep * detected[g, r, b] + leak * (lower + upper)
                for k in range(pblk):
                    counts_ref[b, r, g * group_views:(g + 1) * group_views, k * pb:(k + 1) * pb] = (
                        value[k * group_views:(k + 1) * group_views])

    @pl.when(jnp.logical_not(has_prev))
    def _():
        before[...] = jnp.zeros_like(before)

    @pl.when(jnp.logical_not(has_next))
    def _():
        after[...] = jnp.zeros_like(after)

    multiply(0)
    multiply(1)
    multiply(2)
    add_tiles(0)
    multiply(3)
    add_tiles(1)
    detect(0)
    add_tiles(2)
    detect(1)
    add_tiles(3)
    detect(2)
    detect(3)
    for g in range(GROUPS):
        count(g)
    loop(1, mats, lambda off: copy0(off).wait_send())
    for g in range(GROUPS):
        loop(1, tiles, lambda off: copy1(g, off).wait_send())
        if g < EARLY:
            loop(1, mats, lambda off: copy2(g, off).wait_send())

        @pl.when(has_prev)
        def _():
            copy_down(g).wait_send()

        @pl.when(has_next)
        def _():
            copy_up(g).wait_send()


def per_device(mats, tiles, volume, system, geometry, attenuation, response, crosstalk):
    slices, voxels = volume.shape[1], volume.shape[3]
    views = geometry.shape[1]
    columns, pb = system.shape[2], system.shape[3]
    touch = columns // views
    pblk = PIXELS // pb
    ebins, cbins = attenuation.shape[1], response.shape[0]
    rows = slices // (mats * tiles)
    group_views = views // GROUPS
    rays = group_views * pblk
    assert touch == 2 and pblk == 2 * touch
    vmem = pl.BlockSpec(memory_space=pltpu.VMEM)
    smem = pl.BlockSpec(memory_space=pltpu.SMEM)
    dma = pltpu.SemaphoreType.DMA
    return pl.pallas_call(
        functools.partial(kernel, mats, tiles, slices, voxels, views, touch, pb, pblk, ebins, cbins),
        out_shape=jax.ShapeDtypeStruct((cbins, rows, views, PIXELS), jnp.float32),
        in_specs=[vmem, pl.BlockSpec(memory_space=pl.ANY), smem, smem, smem, smem],
        out_specs=vmem,
        scratch_shapes=[
            pltpu.VMEM((GROUPS, voxels, columns // GROUPS, pb), jnp.bfloat16),
            pltpu.VMEM((mats, slices // mats, voxels), jnp.bfloat16),
            pltpu.VMEM((GROUPS, tiles, mats, rows, columns // GROUPS, pb), jnp.float32),
            pltpu.VMEM((GROUPS, tiles, mats, rows, columns // GROUPS, pb), jnp.float32),
            pltpu.VMEM((GROUPS, mats, rows, rays, pb), jnp.float32),
            pltpu.VMEM((GROUPS, mats, rows, rays, pb), jnp.float32),
            pltpu.VMEM((GROUPS, rows, cbins, rays, pb), jnp.float32),
            pltpu.VMEM((GROUPS, cbins, rays, pb), jnp.float32),
            pltpu.VMEM((GROUPS, cbins, rays, pb), jnp.float32),
            dma((GROUPS,)),
            dma((mats,)),
            dma((mats,)),
            dma((GROUPS, tiles)),
            dma((GROUPS, tiles)),
            dma((GROUPS, mats)),
            dma((GROUPS, mats)),
            dma((GROUPS, 2)),
            dma((GROUPS, 2)),
        ],
        compiler_params=pltpu.CompilerParams(
            collective_id=0, has_side_effects=True, vmem_limit_bytes=60 * 2**20
        ),
        name="project",
    )(volume.reshape(mats, slices // mats, voxels), system.reshape(voxels, columns, pb), geometry, attenuation,
      response, crosstalk)


def solution(mesh):
    in_specs = (P("mat", None, "tile", None), P("tile", None, None, None), P(), P(), P(), P())
    out_specs = P(None, ("mat", "tile"), None, None)
    body = functools.partial(per_device, mesh.shape["mat"], mesh.shape["tile"])
    return jax.shard_map(body, mesh=mesh, in_specs=in_specs, out_specs=out_specs, check_vma=False)
```

```python
import functools

import jax
import jax.numpy as jnp
from jax import lax
from jax.experimental import pallas as pl
from jax.experimental.pallas import tpu as pltpu
from jax.sharding import PartitionSpec as P

PIXELS = 512
GROUPS = 4
EARLY = 2
LOG2E = 1.4426950408889634
MESH = pl.DeviceIdType.MESH


def loop(low, high, body):
    if high - low <= 8:
        for index in range(low, high):
            body(index)
    else:
        lax.fori_loop(low, high, lambda index, _: (body(index), 0)[1], 0)


def kernel(mats, tiles, slices, voxels, views, touch, pb, pblk, ebins, cbins,
           volume_ref, system_ref, geometry_ref, attenuation_ref, response_ref, crosstalk_ref,
           counts_ref,
           matrix, gathered, partial_out, partial_in, summed_out, summed_in, detected, before, after,
           matrix_sem, send0, recv0, send1, recv1, send2, recv2, send3, recv3):
    me_mat, me_tile = lax.axis_index("mat"), lax.axis_index("tile")
    devices = mats * tiles
    me = me_mat * tiles + me_tile
    rows = slices // devices
    group_views = views // GROUPS
    group_cols = group_views * touch
    rays = group_views * pblk
    has_prev, has_next = me > 0, me < devices - 1
    up, down = me + 1, me - 1

    loads = [
        pltpu.make_async_copy(system_ref.at[:, pl.ds(g * group_cols, group_cols)], matrix.at[g], matrix_sem.at[g])
        for g in range(GROUPS)
    ]
    for load in loads:
        load.start()

    barrier = pltpu.get_barrier_semaphore()

    def greet_tile(off):
        pl.semaphore_signal(barrier, inc=1, device_id={"tile": lax.rem(me_tile + off, tiles)}, device_id_type=MESH)

    def greet_mat(off):
        pl.semaphore_signal(barrier, inc=1, device_id={"mat": lax.rem(me_mat + off, mats)}, device_id_type=MESH)

    def place(device):
        return {"mat": device // tiles, "tile": lax.rem(device, tiles)}

    loop(1, tiles, greet_tile)
    loop(1, mats, greet_mat)

    @pl.when(has_prev)
    def _():
        pl.semaphore_signal(barrier, inc=1, device_id=place(down), device_id_type=MESH)

    @pl.when(has_next)
    def _():
        pl.semaphore_signal(barrier, inc=1, device_id=place(up), device_id_type=MESH)

    gathered[me_mat] = volume_ref[me_mat]

    def copy0(off):
        peer = lax.rem(me_mat + off, mats)
        return pltpu.make_async_remote_copy(
            src_ref=volume_ref.at[peer], dst_ref=gathered.at[me_mat],
            send_sem=send0.at[peer], recv_sem=recv0.at[me_mat],
            device_id={"mat": peer}, device_id_type=MESH)

    def arrival0(off):
        peer = lax.rem(me_mat + off, mats)
        return pltpu.make_async_remote_copy(
            src_ref=volume_ref.at[peer], dst_ref=gathered.at[peer],
            send_sem=send0.at[peer], recv_sem=recv0.at[peer],
            device_id={"mat": peer}, device_id_type=MESH)

    known = {}

    def partner(off):
        if isinstance(off, int) and off in known:
            return known[off]
        peer, bit = 0, 1
        while bit < tiles:
            flip = (off // bit) % 2 if isinstance(off, int) else lax.rem(lax.div(off, bit), 2)
            peer += lax.rem(lax.div(me_tile, bit) + flip, 2) * bit
            bit *= 2
        if isinstance(off, int):
            known[off] = peer
        return peer

    def unit(ref, g, slot, part):
        return ref.at[g, slot] if part is None else ref.at[g, slot, part]

    def copy1(g, step, part, arrival=False):
        peer = partner(tiles - step)
        into = peer if arrival else me_tile
        lane = g if part is None else g + part
        return pltpu.make_async_remote_copy(
            src_ref=unit(partial_out, g, peer, part), dst_ref=unit(partial_in, g, into, part),
            send_sem=send1.at[lane, peer], recv_sem=recv1.at[lane, into],
            device_id={"tile": peer}, device_id_type=MESH)

    def parts(g):
        return [None] if g < GROUPS - 1 else list(range(rows))

    def copy2(g, off):
        peer = lax.rem(me_mat + off, mats)
        return pltpu.make_async_remote_copy(
            src_ref=summed_out.at[g, peer], dst_ref=summed_in.at[g, me_mat],
            send_sem=send2.at[g, peer], recv_sem=recv2.at[g, me_mat],
            device_id={"mat": peer}, device_id_type=MESH)

    def arrival2(g, off):
        peer = lax.rem(me_mat + off, mats)
        return pltpu.make_async_remote_copy(
            src_ref=summed_out.at[g, peer], dst_ref=summed_in.at[g, peer],
            send_sem=send2.at[g, peer], recv_sem=recv2.at[g, peer],
            device_id={"mat": peer}, device_id_type=MESH)

    def copy_down(g):
        return pltpu.make_async_remote_copy(
            src_ref=detected.at[g, 0], dst_ref=after.at[g],
            send_sem=send3.at[g, 0], recv_sem=recv3.at[g, 0],
            device_id=place(down), device_id_type=MESH)

    def copy_up(g):
        return pltpu.make_async_remote_copy(
            src_ref=detected.at[g, rows - 1], dst_ref=before.at[g],
            send_sem=send3.at[g, 1], recv_sem=recv3.at[g, 1],
            device_id=place(up), device_id_type=MESH)

    def multiply(g):
        loads[g].wait()
        columns = jnp.swapaxes(matrix[g], 0, 1)
        if g == 0:
            pl.semaphore_wait(
                barrier, tiles - 1 + mats - 1 + has_prev.astype(jnp.int32) + has_next.astype(jnp.int32))
            loop(1, mats, lambda off: copy0(off).start())
        if g == EARLY:
            loop(1, mats, lambda off: arrival0(off).wait_recv())
        source = volume_ref if g < EARLY else gathered
        rows_in = source[...].reshape(slices, voxels)
        products = [None] * group_cols
        for k in range(0, group_cols, 2):
            pair = jnp.concatenate([columns[k], columns[k + 1]], axis=-1)
            product = jnp.dot(rows_in, pair, preferred_element_type=jnp.float32)
            for i in range(2):
                v, j = divmod(k + i, touch)
                products[j * group_views + v] = product[:, i * pb:(i + 1) * pb]
        by_row = jnp.swapaxes(jnp.stack(products, axis=0), 0, 1)
        by_row = by_row.reshape(mats, tiles, rows, group_cols, pb)
        for m in range(mats):
            for r in range(rows):
                partial_out[g, :, r, m] = by_row[m, :, r]
        for part in parts(g):
            loop(1, tiles, lambda step: copy1(g, step, part).start())
        partial_in[g, me_tile] = partial_out[g, me_tile]

    def add_tiles(g, part=None):
        loop(1, tiles, lambda step: copy1(g, step, part, arrival=True).wait_recv())
        picks = list(range(rows)) if part is None else [part]

        sublane = lax.broadcasted_iota(jnp.int32, (group_cols, pb), 0)
        view = lax.rem(sublane, group_views)
        half = sublane < group_views

        def add(tile, sums):
            sums = list(sums)
            first = jnp.full((group_cols, pb), geometry_ref[tile, g * group_views], jnp.int32)
            for v in range(1, group_views):
                first = jnp.where(view == v, geometry_ref[tile, g * group_views + v], first)
            low, middle, high = first == 0, first == 1, first == 2
            low_turned = jnp.logical_and(middle, jnp.logical_not(half))
            high_turned = jnp.logical_and(middle, half)
            for m in range(mats):
                for i, r in enumerate(picks):
                    value = partial_in[g, tile, r, m]
                    turned = jnp.concatenate([value[group_views:], value[:group_views]], axis=0)
                    at = 2 * (m * len(picks) + i)
                    sums[at] += jnp.where(low, value, jnp.where(low_turned, turned, 0.0))
                    sums[at + 1] += jnp.where(high, value, jnp.where(high_turned, turned, 0.0))
            return tuple(sums)

        sums = tuple(jnp.zeros((group_cols, pb), jnp.float32) for _ in range(2 * mats * len(picks)))
        if tiles <= 8:
            for tile in range(tiles):
                sums = add(tile, sums)
        else:
            sums = lax.fori_loop(0, tiles, add, sums)
        target = summed_out if g < EARLY else summed_in
        for m in range(mats):
            for i, r in enumerate(picks):
                at = 2 * (m * len(picks) + i)
                target[g, m, r, :group_cols] = sums[at]
                target[g, m, r, group_cols:] = sums[at + 1]
        if g < EARLY:
            loop(1, mats, lambda off: copy2(g, off).start())
            summed_in[g, me_mat] = summed_out[g, me_mat]

    def detect(g, part=None):
        picks = list(range(rows)) if part is None else [part]
        count_rows = len(picks) * rays
        if g < EARLY:
            loop(1, mats, lambda off: arrival2(g, off).wait_recv())
        scaled = [
            summed_in[g, m, picks[0]:picks[-1] + 1].reshape(count_rows, pb) * (-LOG2E) for m in range(mats)
        ]
        unroll = 8

        def energies(block, totals):
            totals = list(totals)
            for inner in range(unroll):
                e = block * unroll + inner
                power = attenuation_ref[0, e] * scaled[0]
                for m in range(1, mats):
                    power += attenuation_ref[m, e] * scaled[m]
                passed = jnp.exp2(power)
                for b in range(cbins):
                    totals[b] += response_ref[b, e] * passed
            return tuple(totals)

        totals = tuple(jnp.zeros((count_rows, pb), jnp.float32) for _ in range(cbins))
        totals = lax.fori_loop(0, ebins // unroll, energies, totals)
        for b in range(cbins):
            for i, r in enumerate(picks):
                detected[g, r, b] = totals[b][i * rays:(i + 1) * rays]

        if 0 in picks:
            @pl.when(has_prev)
            def _():
                copy_down(g).start()

        if rows - 1 in picks:
            @pl.when(has_next)
            def _():
                copy_up(g).start()

    def count(g):
        @pl.when(has_prev)
        def _():
            copy_up(g).wait_recv()

        @pl.when(has_next)
        def _():
            copy_down(g).wait_recv()

        for b in range(cbins):
            leak = crosstalk_ref[b]
            keep = 1.0 - 2.0 * leak
            for r in range(rows):
                lower = detected[g, r - 1, b] if r > 0 else before[g, b]
                upper = detected[g, r + 1, b] if r < rows - 1 else after[g, b]
                value = keep * detected[g, r, b] + leak * (lower + upper)
                for k in range(pblk):
                    counts_ref[b, r, g * group_views:(g + 1) * group_views, k * pb:(k + 1) * pb] = (
                        value[k * group_views:(k + 1) * group_views])

    @pl.when(jnp.logical_not(has_prev))
    def _():
        before[...] = jnp.zeros_like(before)

    @pl.when(jnp.logical_not(has_next))
    def _():
        after[...] = jnp.zeros_like(after)

    for g in range(GROUPS):
        multiply(g)
    for g in range(EARLY):
        add_tiles(g)
    for g in range(EARLY):
        detect(g)
    for g in range(EARLY, GROUPS - 1):
        add_tiles(g)
        detect(g)
    for g in range(EARLY):
        count(g)
    for part in parts(GROUPS - 1):
        add_tiles(GROUPS - 1, part)
        detect(GROUPS - 1, part)
    for g in range(EARLY, GROUPS):
        count(g)
    loop(1, mats, lambda off: copy0(off).wait_send())
    for g in range(GROUPS):
        for part in parts(g):
            loop(1, tiles, lambda step: copy1(g, step, part).wait_send())
        if g < EARLY:
            loop(1, mats, lambda off: copy2(g, off).wait_send())

        @pl.when(has_prev)
        def _():
            copy_down(g).wait_send()

        @pl.when(has_next)
        def _():
            copy_up(g).wait_send()


def per_device(mats, tiles, volume, system, geometry, attenuation, response, crosstalk):
    slices, voxels = volume.shape[1], volume.shape[3]
    views = geometry.shape[1]
    columns, pb = system.shape[2], system.shape[3]
    touch = columns // views
    pblk = PIXELS // pb
    ebins, cbins = attenuation.shape[1], response.shape[0]
    rows = slices // (mats * tiles)
    group_views = views // GROUPS
    rays = group_views * pblk
    assert touch == 2 and pblk == 2 * touch
    vmem = pl.BlockSpec(memory_space=pltpu.VMEM)
    smem = pl.BlockSpec(memory_space=pltpu.SMEM)
    dma = pltpu.SemaphoreType.DMA
    return pl.pallas_call(
        functools.partial(kernel, mats, tiles, slices, voxels, views, touch, pb, pblk, ebins, cbins),
        out_shape=jax.ShapeDtypeStruct((cbins, rows, views, PIXELS), jnp.float32),
        in_specs=[vmem, pl.BlockSpec(memory_space=pl.ANY), smem, smem, smem, smem],
        out_specs=vmem,
        scratch_shapes=[
            pltpu.VMEM((GROUPS, voxels, columns // GROUPS, pb), jnp.bfloat16),
            pltpu.VMEM((mats, slices // mats, voxels), jnp.bfloat16),
            pltpu.VMEM((GROUPS, tiles, rows, mats, columns // GROUPS, pb), jnp.float32),
            pltpu.VMEM((GROUPS, tiles, rows, mats, columns // GROUPS, pb), jnp.float32),
            pltpu.VMEM((GROUPS, mats, rows, rays, pb), jnp.float32),
            pltpu.VMEM((GROUPS, mats, rows, rays, pb), jnp.float32),
            pltpu.VMEM((GROUPS, rows, cbins, rays, pb), jnp.float32),
            pltpu.VMEM((GROUPS, cbins, rays, pb), jnp.float32),
            pltpu.VMEM((GROUPS, cbins, rays, pb), jnp.float32),
            dma((GROUPS,)),
            dma((mats,)),
            dma((mats,)),
            dma((GROUPS + rows - 1, tiles)),
            dma((GROUPS + rows - 1, tiles)),
            dma((GROUPS, mats)),
            dma((GROUPS, mats)),
            dma((GROUPS, 2)),
            dma((GROUPS, 2)),
        ],
        compiler_params=pltpu.CompilerParams(
            collective_id=0, has_side_effects=True, vmem_limit_bytes=60 * 2**20
        ),
        name="project",
    )(volume.reshape(mats, slices // mats, voxels), system.reshape(voxels, columns, pb), geometry, attenuation,
      response, crosstalk)


def solution(mesh):
    in_specs = (P("mat", None, "tile", None), P("tile", None, None, None), P(), P(), P(), P())
    out_specs = P(None, ("mat", "tile"), None, None)
    body = functools.partial(per_device, mesh.shape["mat"], mesh.shape["tile"])
    return jax.shard_map(body, mesh=mesh, in_specs=in_specs, out_specs=out_specs, check_vma=False)
```

```python
import functools

import jax
import jax.numpy as jnp
from jax import lax
from jax.experimental import pallas as pl
from jax.experimental.pallas import tpu as pltpu
from jax.sharding import PartitionSpec as P

PIXELS = 512
GROUPS = 4
EARLY = 2
LOG2E = 1.4426950408889634
MESH = pl.DeviceIdType.MESH


def loop(low, high, body):
    if high - low <= 8:
        for index in range(low, high):
            body(index)
    else:
        lax.fori_loop(low, high, lambda index, _: (body(index), 0)[1], 0)


def kernel(mats, tiles, slices, voxels, views, touch, pb, pblk, ebins, cbins,
           volume_ref, system_ref, geometry_ref, attenuation_ref, response_ref, crosstalk_ref,
           counts_ref,
           matrix, gathered, partial_out, partial_in, summed_out, summed_in, detected, before, after,
           matrix_sem, send0, recv0, send1, recv1, send2, recv2, send3, recv3):
    me_mat, me_tile = lax.axis_index("mat"), lax.axis_index("tile")
    devices = mats * tiles
    me = me_mat * tiles + me_tile
    rows = slices // devices
    group_views = views // GROUPS
    group_cols = group_views * touch
    rays = group_views * pblk
    has_prev, has_next = me > 0, me < devices - 1
    up, down = me + 1, me - 1

    loads = [
        pltpu.make_async_copy(system_ref.at[:, pl.ds(g * group_cols, group_cols)], matrix.at[g], matrix_sem.at[g])
        for g in range(GROUPS)
    ]
    for load in loads:
        load.start()

    barrier = pltpu.get_barrier_semaphore()

    def greet_tile(off):
        pl.semaphore_signal(barrier, inc=1, device_id={"tile": lax.rem(me_tile + off, tiles)}, device_id_type=MESH)

    def greet_mat(off):
        pl.semaphore_signal(barrier, inc=1, device_id={"mat": lax.rem(me_mat + off, mats)}, device_id_type=MESH)

    def place(device):
        return {"mat": device // tiles, "tile": lax.rem(device, tiles)}

    loop(1, tiles, greet_tile)
    loop(1, mats, greet_mat)

    @pl.when(has_prev)
    def _():
        pl.semaphore_signal(barrier, inc=1, device_id=place(down), device_id_type=MESH)

    @pl.when(has_next)
    def _():
        pl.semaphore_signal(barrier, inc=1, device_id=place(up), device_id_type=MESH)

    gathered[me_mat] = volume_ref[me_mat]

    def copy0(off):
        peer = lax.rem(me_mat + off, mats)
        return pltpu.make_async_remote_copy(
            src_ref=volume_ref.at[peer], dst_ref=gathered.at[me_mat],
            send_sem=send0.at[peer], recv_sem=recv0.at[me_mat],
            device_id={"mat": peer}, device_id_type=MESH)

    def arrival0(off):
        peer = lax.rem(me_mat + off, mats)
        return pltpu.make_async_remote_copy(
            src_ref=volume_ref.at[peer], dst_ref=gathered.at[peer],
            send_sem=send0.at[peer], recv_sem=recv0.at[peer],
            device_id={"mat": peer}, device_id_type=MESH)

    def unit(ref, g, slot, part):
        return ref.at[g, slot] if part is None else ref.at[g, slot, part]

    def copy1(g, step, part, arrival=False):
        peer = lax.rem(me_tile + step, tiles)
        into = peer if arrival else me_tile
        lane = g if part is None else g + part
        return pltpu.make_async_remote_copy(
            src_ref=unit(partial_out, g, peer, part), dst_ref=unit(partial_in, g, into, part),
            send_sem=send1.at[lane, peer], recv_sem=recv1.at[lane, into],
            device_id={"tile": peer}, device_id_type=MESH)

    def parts(g):
        return [None] if g < GROUPS - 1 else list(range(rows))

    def copy2(g, off):
        peer = lax.rem(me_mat + off, mats)
        return pltpu.make_async_remote_copy(
            src_ref=summed_out.at[g, peer], dst_ref=summed_in.at[g, me_mat],
            send_sem=send2.at[g, peer], recv_sem=recv2.at[g, me_mat],
            device_id={"mat": peer}, device_id_type=MESH)

    def arrival2(g, off):
        peer = lax.rem(me_mat + off, mats)
        return pltpu.make_async_remote_copy(
            src_ref=summed_out.at[g, peer], dst_ref=summed_in.at[g, peer],
            send_sem=send2.at[g, peer], recv_sem=recv2.at[g, peer],
            device_id={"mat": peer}, device_id_type=MESH)

    def copy_down(g):
        return pltpu.make_async_remote_copy(
            src_ref=detected.at[g, 0], dst_ref=after.at[g],
            send_sem=send3.at[g, 0], recv_sem=recv3.at[g, 0],
            device_id=place(down), device_id_type=MESH)

    def copy_up(g):
        return pltpu.make_async_remote_copy(
            src_ref=detected.at[g, rows - 1], dst_ref=before.at[g],
            send_sem=send3.at[g, 1], recv_sem=recv3.at[g, 1],
            device_id=place(up), device_id_type=MESH)

    def multiply(g):
        loads[g].wait()
        columns = jnp.swapaxes(matrix[g], 0, 1)
        if g == 0:
            pl.semaphore_wait(
                barrier, tiles - 1 + mats - 1 + has_prev.astype(jnp.int32) + has_next.astype(jnp.int32))
            loop(1, mats, lambda off: copy0(off).start())
        if g == EARLY:
            loop(1, mats, lambda off: arrival0(off).wait_recv())
        source = volume_ref if g < EARLY else gathered
        rows_in = source[...].reshape(slices, voxels)
        products = [None] * group_cols
        for k in range(0, group_cols, 2):
            pair = jnp.concatenate([columns[k], columns[k + 1]], axis=-1)
            product = jnp.dot(rows_in, pair, preferred_element_type=jnp.float32)
            for i in range(2):
                v, j = divmod(k + i, touch)
                products[j * group_views + v] = product[:, i * pb:(i + 1) * pb]
        by_row = jnp.swapaxes(jnp.stack(products, axis=0), 0, 1)
        by_row = by_row.reshape(mats, tiles, rows, group_cols, pb)
        for m in range(mats):
            for r in range(rows):
                partial_out[g, :, r, m] = by_row[m, :, r]
        for part in parts(g):
            loop(1, tiles, lambda step: copy1(g, step, part).start())
        partial_in[g, me_tile] = partial_out[g, me_tile]

    def add_tiles(g, part=None):
        loop(1, tiles, lambda step: copy1(g, step, part, arrival=True).wait_recv())
        picks = list(range(rows)) if part is None else [part]

        sublane = lax.broadcasted_iota(jnp.int32, (group_cols, pb), 0)
        view = lax.rem(sublane, group_views)
        half = sublane < group_views

        def add(tile, sums):
            sums = list(sums)
            first = jnp.full((group_cols, pb), geometry_ref[tile, g * group_views], jnp.int32)
            for v in range(1, group_views):
                first = jnp.where(view == v, geometry_ref[tile, g * group_views + v], first)
            low, middle, high = first == 0, first == 1, first == 2
            low_turned = jnp.logical_and(middle, jnp.logical_not(half))
            high_turned = jnp.logical_and(middle, half)
            for m in range(mats):
                for i, r in enumerate(picks):
                    value = partial_in[g, tile, r, m]
                    turned = jnp.concatenate([value[group_views:], value[:group_views]], axis=0)
                    at = 2 * (m * len(picks) + i)
                    sums[at] += jnp.where(low, value, jnp.where(low_turned, turned, 0.0))
                    sums[at + 1] += jnp.where(high, value, jnp.where(high_turned, turned, 0.0))
            return tuple(sums)

        sums = tuple(jnp.zeros((group_cols, pb), jnp.float32) for _ in range(2 * mats * len(picks)))
        if tiles <= 8:
            for tile in range(tiles):
                sums = add(tile, sums)
        else:
            sums = lax.fori_loop(0, tiles, add, sums)
        target = summed_out if g < EARLY else summed_in
        for m in range(mats):
            for i, r in enumerate(picks):
                at = 2 * (m * len(picks) + i)
                target[g, m, r, :group_cols] = sums[at]
                target[g, m, r, group_cols:] = sums[at + 1]
        if g < EARLY:
            loop(1, mats, lambda off: copy2(g, off).start())
            summed_in[g, me_mat] = summed_out[g, me_mat]

    def detect(g, part=None):
        picks = list(range(rows)) if part is None else [part]
        count_rows = len(picks) * rays
        if g < EARLY:
            loop(1, mats, lambda off: arrival2(g, off).wait_recv())
        scaled = [
            summed_in[g, m, picks[0]:picks[-1] + 1].reshape(count_rows, pb) * (-LOG2E) for m in range(mats)
        ]
        unroll = 8

        def energies(block, totals):
            totals = list(totals)
            for inner in range(unroll):
                e = block * unroll + inner
                power = attenuation_ref[0, e] * scaled[0]
                for m in range(1, mats):
                    power += attenuation_ref[m, e] * scaled[m]
                passed = jnp.exp2(power)
                for b in range(cbins):
                    totals[b] += response_ref[b, e] * passed
            return tuple(totals)

        totals = tuple(jnp.zeros((count_rows, pb), jnp.float32) for _ in range(cbins))
        totals = lax.fori_loop(0, ebins // unroll, energies, totals)
        for b in range(cbins):
            for i, r in enumerate(picks):
                detected[g, r, b] = totals[b][i * rays:(i + 1) * rays]

        if 0 in picks:
            @pl.when(has_prev)
            def _():
                copy_down(g).start()

        if rows - 1 in picks:
            @pl.when(has_next)
            def _():
                copy_up(g).start()

    def count(g):
        @pl.when(has_prev)
        def _():
            copy_up(g).wait_recv()

        @pl.when(has_next)
        def _():
            copy_down(g).wait_recv()

        for b in range(cbins):
            leak = crosstalk_ref[b]
            keep = 1.0 - 2.0 * leak
            for r in range(rows):
                lower = detected[g, r - 1, b] if r > 0 else before[g, b]
                upper = detected[g, r + 1, b] if r < rows - 1 else after[g, b]
                value = keep * detected[g, r, b] + leak * (lower + upper)
                for k in range(pblk):
                    counts_ref[b, r, g * group_views:(g + 1) * group_views, k * pb:(k + 1) * pb] = (
                        value[k * group_views:(k + 1) * group_views])

    @pl.when(jnp.logical_not(has_prev))
    def _():
        before[...] = jnp.zeros_like(before)

    @pl.when(jnp.logical_not(has_next))
    def _():
        after[...] = jnp.zeros_like(after)

    for g in range(GROUPS):
        multiply(g)
    for g in range(EARLY):
        add_tiles(g)
    for g in range(EARLY):
        detect(g)
    for g in range(EARLY, GROUPS - 1):
        add_tiles(g)
        detect(g)
    for g in range(EARLY):
        count(g)
    for part in parts(GROUPS - 1):
        add_tiles(GROUPS - 1, part)
        detect(GROUPS - 1, part)
    for g in range(EARLY, GROUPS):
        count(g)
    loop(1, mats, lambda off: copy0(off).wait_send())
    for g in range(GROUPS):
        for part in parts(g):
            loop(1, tiles, lambda step: copy1(g, step, part).wait_send())
        if g < EARLY:
            loop(1, mats, lambda off: copy2(g, off).wait_send())

        @pl.when(has_prev)
        def _():
            copy_down(g).wait_send()

        @pl.when(has_next)
        def _():
            copy_up(g).wait_send()


def per_device(mats, tiles, volume, system, geometry, attenuation, response, crosstalk):
    slices, voxels = volume.shape[1], volume.shape[3]
    views = geometry.shape[1]
    columns, pb = system.shape[2], system.shape[3]
    touch = columns // views
    pblk = PIXELS // pb
    ebins, cbins = attenuation.shape[1], response.shape[0]
    rows = slices // (mats * tiles)
    group_views = views // GROUPS
    rays = group_views * pblk
    assert touch == 2 and pblk == 2 * touch
    vmem = pl.BlockSpec(memory_space=pltpu.VMEM)
    smem = pl.BlockSpec(memory_space=pltpu.SMEM)
    dma = pltpu.SemaphoreType.DMA
    return pl.pallas_call(
        functools.partial(kernel, mats, tiles, slices, voxels, views, touch, pb, pblk, ebins, cbins),
        out_shape=jax.ShapeDtypeStruct((cbins, rows, views, PIXELS), jnp.float32),
        in_specs=[vmem, pl.BlockSpec(memory_space=pl.ANY), smem, smem, smem, smem],
        out_specs=vmem,
        scratch_shapes=[
            pltpu.VMEM((GROUPS, voxels, columns // GROUPS, pb), jnp.bfloat16),
            pltpu.VMEM((mats, slices // mats, voxels), jnp.bfloat16),
            pltpu.VMEM((GROUPS, tiles, rows, mats, columns // GROUPS, pb), jnp.float32),
            pltpu.VMEM((GROUPS, tiles, rows, mats, columns // GROUPS, pb), jnp.float32),
            pltpu.VMEM((GROUPS, mats, rows, rays, pb), jnp.float32),
            pltpu.VMEM((GROUPS, mats, rows, rays, pb), jnp.float32),
            pltpu.VMEM((GROUPS, rows, cbins, rays, pb), jnp.float32),
            pltpu.VMEM((GROUPS, cbins, rays, pb), jnp.float32),
            pltpu.VMEM((GROUPS, cbins, rays, pb), jnp.float32),
            dma((GROUPS,)),
            dma((mats,)),
            dma((mats,)),
            dma((GROUPS + rows - 1, tiles)),
            dma((GROUPS + rows - 1, tiles)),
            dma((GROUPS, mats)),
            dma((GROUPS, mats)),
            dma((GROUPS, 2)),
            dma((GROUPS, 2)),
        ],
        compiler_params=pltpu.CompilerParams(
            collective_id=0, has_side_effects=True, vmem_limit_bytes=60 * 2**20
        ),
        name="project",
    )(volume.reshape(mats, slices // mats, voxels), system.reshape(voxels, columns, pb), geometry, attenuation,
      response, crosstalk)


def solution(mesh):
    in_specs = (P("mat", None, "tile", None), P("tile", None, None, None), P(), P(), P(), P())
    out_specs = P(None, ("mat", "tile"), None, None)
    body = functools.partial(per_device, mesh.shape["mat"], mesh.shape["tile"])
    return jax.shard_map(body, mesh=mesh, in_specs=in_specs, out_specs=out_specs, check_vma=False)
```
